32 devices in a mesh: group: 1, stream: 16 (over z, y, x), expert: 2 (over core).
Axes of the slice: x: 2, y: 2, z: 4, core: 2. Of those that a mesh axis runs over, the one named last changes fastest.
Arguments:
- hidden_in: bfloat16 [512, 4096], P(('group', 'stream', 'expert')), may hold values from -6 to 6
- routes: int32 [512, 2], P(('group', 'stream', 'expert')), may hold values from 0 to 3, all different within a row; in each aligned block of 512 rows (0 to 511, 512 to 1023, ...) at most 384 rows name the same one
- norm_gain: float32 [4096], replicated, may hold values from 0.25 to 1.75
- router: bfloat16 [4096, 4], replicated, may hold values from -0.1875 to 0.1875
- w_gate: bfloat16 [4, 4096, 7168], P('expert', None, 'stream'), may hold values from -0.09375 to 0.09375
- w_up: bfloat16 [4, 4096, 7168], P('expert', None, 'stream'), may hold values from -0.09375 to 0.09375
- w_down: bfloat16 [4, 7168, 4096], P('expert', 'stream'), may hold values from -0.0625 to 0.0625
Outputs:
- hidden_out: bfloat16 [512, 4096], P(('group', 'stream', 'expert'))
The draws below stay inside these ranges and needn't reach their ends.
Inputs may be any that keep to these rules, and one draw needn't show every extreme that they name: `routes`: each token names two different experts; no expert is named by more than 384 tokens of a replica, a bound that some block reaches.
All inputs are finite; a program needn't handle non-finite values.
Results may differ from the reference program's by a relative error of at most 0.006.
Values may be sent and summed in bfloat16 or wider, within the bound.
A program may use at most 192 MiB of HBM per device.

```python
import math
import jax
import jax.numpy as jnp
import numpy as np
from jax import lax

D = 4096
FF = 7168
EXPERTS = 4
TOKENS = 512
CAP = 384


def shard_levels(stream_key, shape, shards, smallest, top_value):
    loudness = 1.0
    for dim, shards_of in shards:
        steps = jax.random.uniform(jax.random.fold_in(jax.random.fold_in(stream_key, 6), dim), (shards_of,), jnp.float32, smallest / len(shards), top_value / len(shards))
        loudness = loudness * jnp.repeat(jnp.exp(steps), shape[dim] // shards_of).reshape((-1,) + (1,) * (len(shape) - 1 - dim))
    return loudness


def assign_block(stream_key, own, number, rows, number_of, top, bound, skew):
    ranking = jax.random.permutation(stream_key, number_of)
    crowded, ordinary = shares(number_of, rows * top, bound, skew, True), shares(number_of, rows * top, bound, skew, False)
    places = jnp.arange(number_of)

    def named(tallies, rotation):
        used = int((tallies > 0).sum())
        fixed = max(1, used // 4)
        passed = fixed + (places - fixed + rotation * (used - fixed)) % max(1, number_of - fixed)
        return jnp.zeros((number_of,), jnp.int32).at[ranking[jnp.where(places < fixed, places, passed)]].set(jnp.asarray(tallies, jnp.int32))

    tallies = jnp.where(number % 4 == 0, named(crowded, number // 4), named(ordinary, number - number // 4 - 1))
    mixed = jax.random.permutation(jax.random.fold_in(own, 3), number_of)
    source_of, receiver = mixed[0:number_of // 2 * 2:2], mixed[1:number_of // 2 * 2:2]
    slack = jnp.minimum(tallies[source_of] - 1, bound - tallies[receiver]) // 2
    slack = jnp.where((source_of == ranking[0]) | (receiver == ranking[0]) | (tallies[receiver] == 0), 0, jnp.maximum(slack, 0))
    passed = jax.random.randint(jax.random.fold_in(own, 4), (number_of // 2,), 0, 1 << 20) % (slack + 1)
    tallies = tallies.at[source_of].add(-passed).at[receiver].add(passed)
    items = jnp.searchsorted(jnp.cumsum(tallies), jnp.arange(rows * top), side="right").astype(jnp.int32)
    listing = items.reshape(top, rows).T
    listing = listing[jax.random.permutation(jax.random.fold_in(own, 1), rows)]
    rotation = jax.random.randint(jax.random.fold_in(own, 2), (rows, 1), 0, top)
    return jnp.take_along_axis(listing, (jnp.arange(top)[None, :] + rotation) % top, axis=1)


def shares(count, total, bound, slope, full):
    weights = [(1 << 20) // math.isqrt(standing ** slope) + 1 for standing in range(1, count + 1)]
    largest = bound if full else min(bound, max(-(-total // count), total * weights[0] // sum(weights)))
    least = 1 if total - largest >= count - 1 else 0
    given, surplus = [largest] + [least] * (count - 1), total - largest - least * (count - 1)
    while surplus > 0:
        free = [i for i in range(1, count) if given[i] < largest] or [i for i in range(1, count) if given[i] < bound]
        whole, budget = sum([weights[i] for i in free]), surplus
        for i in free:
            addition = min(bound - given[i], max(1, budget * weights[i] // whole), surplus)
            given[i] = given[i] + addition
            surplus = surplus - addition
    return np.array(given)


def bell_draw(key, shape, scale, bound, pieces=(), kind=jnp.bfloat16):
    array = jax.random.normal(key, shape, jnp.float32) * scale
    if len(pieces) > 0:
        array = shard_levels(key, shape, pieces, -0.22, 0.18) * array
    return jnp.clip(array, min=-bound, max=bound).astype(kind)


def setup_inputs(seed: int = 0, part: int = 0) -> dict:
    streams_of = jax.random.split(jax.random.key(seed), 8)
    own_keys = jax.random.split(jax.random.fold_in(streams_of[7], part), 8)
    hidden_in = bell_draw(own_keys[0], (TOKENS, D), 1.0, 6.0, ((0, 32),))
    routes_keys = jax.random.split(jax.random.fold_in(own_keys[1], 1), TOKENS // TOKENS)
    routes_turns = jax.random.permutation(jax.random.fold_in(own_keys[1], 3), TOKENS // TOKENS)
    routes = jax.vmap(lambda own, number: assign_block(jax.random.fold_in(own_keys[1], 2), own, number, TOKENS, EXPERTS, 2, CAP, 1))(routes_keys, routes_turns).reshape((TOKENS, 2))
    norm_gain = jnp.clip(1.0 + 0.15 * jax.random.normal(streams_of[2], (D,), jnp.float32), 0.25, 1.75)
    router = bell_draw(streams_of[3], (D, EXPERTS), (D // 4) ** -0.5, 0.1875)
    w_gate = bell_draw(streams_of[4], (EXPERTS, D, FF), D ** -0.5, 0.09375, ((0, 2), (2, 16)))
    w_up = bell_draw(streams_of[5], (EXPERTS, D, FF), D ** -0.5, 0.09375, ((0, 2), (2, 16)))
    w_down = bell_draw(streams_of[6], (EXPERTS, FF, D), FF ** -0.5, 0.0625, ((0, 2), (1, 16)))
    return {"hidden_in": hidden_in, "routes": routes, "norm_gain": norm_gain, "router": router, "w_gate": w_gate, "w_up": w_up, "w_down": w_down}


EPS = 1e-05

def route_table(normed, routes, router):
    logits = jnp.dot(normed, router, preferred_element_type=jnp.float32)
    picked = jnp.take_along_axis(logits, routes, axis=1)
    first_weight = 1.0 / (1.0 + jnp.exp(picked[:, 1] - picked[:, 0]))
    second_weight = 1.0 - first_weight
    experts = jnp.arange(router.shape[1], dtype=jnp.int32)
    table = jnp.where(routes[:, 0:1] == experts, first_weight[:, None], jnp.zeros((), jnp.float32))
    table = table + jnp.where(routes[:, 1:2] == experts, second_weight[:, None], jnp.zeros((), jnp.float32))
    return table.astype(jnp.bfloat16)

def reference(hidden_in, routes, norm_gain, router, w_gate, w_up, w_down):
    own_rows = hidden_in.astype(jnp.float32)
    mean_sq = lax.optimization_barrier(jnp.mean(own_rows * own_rows, axis=1, keepdims=True))
    normed = (own_rows * lax.rsqrt(mean_sq + EPS) * norm_gain).astype(jnp.bfloat16)
    route_weights = route_table(normed, routes, router)
    row_total = normed.shape[0]
    position = jnp.arange(row_total, dtype=jnp.int32)
    mixture = jnp.zeros(own_rows.shape, jnp.float32)
    for expert_slot in range(EXPERTS):
        weight = route_weights[:, expert_slot].astype(jnp.float32)
        sort_keys = jnp.where(weight > 0, position, position + row_total)
        chosen = jnp.argsort(sort_keys)[:CAP]
        rows = normed[chosen]
        gate_proj = jnp.dot(rows, w_gate[expert_slot], preferred_element_type=jnp.float32)
        up_proj = jnp.dot(rows, w_up[expert_slot], preferred_element_type=jnp.float32)
        activated = (jax.nn.silu(gate_proj) * up_proj).astype(jnp.bfloat16)
        expert_out = jnp.dot(activated, w_down[expert_slot], preferred_element_type=jnp.float32)
        mixture = mixture.at[chosen].add(expert_out * weight[chosen][:, None])
    return (own_rows + mixture).astype(jnp.bfloat16)
```

```python
import functools

import jax
import jax.numpy as jnp
from jax import lax
from jax.experimental import pallas as pl
from jax.experimental.pallas import tpu as pltpu
from jax.sharding import PartitionSpec as P

EPS = 1e-05
LANES = 128
MESH = pl.DeviceIdType.MESH


def kernel(
    sizes,
    hidden_ref,
    routes_ref,
    gain_ref,
    router_ref,
    gate_hbm,
    up_hbm,
    down_hbm,
    out_ref,
    w_in,
    w_out,
    rows_buf,
    acc,
    act,
    part,
    send_d,
    recv_d,
    send_q,
    recv_q,
    send_p,
    recv_p,
    send_z,
    recv_z,
    send_sems,
    recv_sems,
    load_sems,
):
    depth, chunks, width, own = sizes
    features = chunks * width
    local = w_in.shape[1]
    total = rows_buf.shape[0]
    half, quarter, eighth = total // 2, total // 4, total // 8
    per_item = depth - 1 + 3

    group = lax.axis_index("group")
    s = lax.axis_index("stream")
    e = lax.axis_index("expert")
    z = s // 4
    b = (s // 2) % 2
    a = s % 2
    p = b * (1 - e) + a * e
    q = a * (1 - e) + b * e
    peer_p = (group, s + (1 - 2 * p) * (2 - e), e)
    peer_q = (group, s + (1 - 2 * q) * (1 + e), e)
    peer_d = (group, s, 1 - e)

    def peer_z(d):
        return (group, s + ((z + d) % depth - z) * 4, e)

    barrier = pltpu.get_barrier_semaphore()
    everyone = [peer_z(d) for d in range(1, depth)] + [peer_p, peer_q, peer_d]
    for peer in everyone:
        pl.semaphore_signal(barrier, inc=1, device_id=peer, device_id_type=MESH)

    loads = []
    for c in range(chunks):
        ks = pl.ds(c * width, width)
        loads.append(
            (
                pltpu.make_async_copy(gate_hbm.at[:, ks, :], w_in.at[0, :, ks, :], load_sems.at[3 * c]),
                pltpu.make_async_copy(up_hbm.at[:, ks, :], w_in.at[1, :, ks, :], load_sems.at[3 * c + 1]),
            )
        )
    for c in range(chunks):
        ks = pl.ds(c * width, width)
        loads.append(
            (pltpu.make_async_copy(down_hbm.at[:, :, ks], w_out.at[:, :, ks], load_sems.at[3 * c + 2]),)
        )
    for pair in loads:
        for load in pair:
            load.start()

    def at(index, step):
        return pl.ds(pl.multiple_of(index * step, step), step)

    own_rows = hidden_ref[...].astype(jnp.float32)
    mean_sq = jnp.mean(own_rows * own_rows, axis=1, keepdims=True)
    normed = (own_rows * lax.rsqrt(mean_sq + EPS) * gain_ref[...]).astype(jnp.bfloat16)
    normed32 = normed.astype(jnp.float32)
    first = routes_ref[:, 0:1]
    second = routes_ref[:, 1:2]
    first_logit = jnp.zeros((own, 1), jnp.float32)
    second_logit = jnp.zeros((own, 1), jnp.float32)
    for x in range(router_ref.shape[0]):
        logit = jnp.sum(normed32 * router_ref[x : x + 1, :].astype(jnp.float32), axis=1, keepdims=True)
        first_logit = jnp.where(first == x, logit, first_logit)
        second_logit = jnp.where(second == x, logit, second_logit)
    first_weight = 1.0 / (1.0 + jnp.exp(second_logit - first_logit))
    second_weight = 1.0 - first_weight
    lane = lax.broadcasted_iota(jnp.int32, (own, LANES), 1)
    table = jnp.where(lane == first, first_weight, 0.0) + jnp.where(lane == second, second_weight, 0.0)
    block = ((e * 2 + q) * 2 + p) * depth + z
    rows_buf[at(block, own), 0:features] = normed
    rows_buf[at(block, own), features : features + LANES] = table.astype(jnp.bfloat16)

    pl.semaphore_wait(barrier, depth - 1 + 3)

    def remote(slot, src, dst, peer):
        return pltpu.make_async_remote_copy(
            src_ref=src,
            dst_ref=dst,
            send_sem=send_sems.at[slot],
            recv_sem=recv_sems.at[slot],
            device_id=peer,
            device_id_type=MESH,
        )

    started = []

    def go(copy):
        copy.start()
        started.append(copy)

    def cols_of(c):
        extra = LANES if c == chunks - 1 else 0
        return pl.ds(c * width, width + extra)

    def gather_z(c, d):
        view = rows_buf.at[at(block, own), cols_of(c)]
        return remote(c * per_item + d - 1, view, view, peer_z(d))

    def gather_p(c):
        view = rows_buf.at[at((e * 2 + q) * 2 + p, eighth), cols_of(c)]
        return remote(c * per_item + depth - 1, view, view, peer_p)

    def gather_q(c):
        view = rows_buf.at[at(e * 2 + q, quarter), cols_of(c)]
        return remote(c * per_item + depth, view, view, peer_q)

    def gather_d(c):
        view = rows_buf.at[at(e, half), cols_of(c)]
        return remote(c * per_item + depth + 1, view, view, peer_d)

    mrows = min(total, 512)
    mcount = total // mrows

    def multiply(c):
        for load in loads[c]:
            load.wait()
        ks = pl.ds(c * width, width)

        def step(i, carry):
            m = i % mcount
            j = i // mcount
            rows = pl.ds(pl.multiple_of(m * mrows, mrows), mrows)
            product = jnp.dot(
                rows_buf[rows, ks], w_in[j // local, j % local, ks, :], preferred_element_type=jnp.float32
            )
            if c == 0:
                acc[j, rows, :] = product
            else:
                acc[j, rows, :] += product
            return carry

        lax.fori_loop(0, 2 * local * mcount, step, 0)

    for c in range(chunks):
        for d in range(1, depth):
            go(gather_z(c, d))
    for t in range(chunks + 3):
        if t < chunks:
            for d in range(1, depth):
                gather_z(t, d).wait_recv()
            go(gather_p(t))
        if 0 <= t - 1 < chunks:
            gather_p(t - 1).wait_recv()
            go(gather_q(t - 1))
        if 0 <= t - 2 < chunks:
            gather_q(t - 2).wait_recv()
            go(gather_d(t - 2))
        if 0 <= t - 3 < chunks:
            gather_d(t - 3).wait_recv()
            multiply(t - 3)

    arows = 128

    def activate(i, carry):
        x = i % local
        rows = pl.ds(pl.multiple_of((i // local) * arows, arows), arows)
        expert = e * local + x
        weights = rows_buf[rows, features : features + LANES].astype(jnp.float32)
        lanes = lax.broadcasted_iota(jnp.int32, (arows, LANES), 1)
        weight = jnp.sum(jnp.where(lanes == expert, weights, 0.0), axis=1, keepdims=True)
        gate = acc[x, rows, :]
        up = acc[local + x, rows, :]
        act[x, rows, :] = (gate / (1.0 + jnp.exp(-gate)) * up * weight).astype(jnp.bfloat16)
        return carry

    lax.fori_loop(0, local * (total // arows), activate, 0)

    base = chunks * per_item
    tile = 256
    row_q = q * quarter
    row_p = q * quarter + p * eighth

    def down(rows, cols):
        result = jnp.dot(act[0, rows, :], w_out[0, :, cols], preferred_element_type=jnp.float32)
        for x in range(1, local):
            result += jnp.dot(act[x, rows, :], w_out[x, :, cols], preferred_element_type=jnp.float32)
        return result

    def reduce_d(n):
        return remote(base + n * per_item + depth + 1, send_d.at[n], recv_d.at[n], peer_d)

    def reduce_q(n):
        return remote(base + n * per_item + depth, send_q.at[n], recv_q.at[n], peer_q)

    def reduce_p(n):
        return remote(base + n * per_item + depth - 1, send_p.at[n], recv_p.at[n], peer_p)

    def reduce_z(n, d):
        view = send_z.at[n, at((z + d) % depth, own), :]
        return remote(base + n * per_item + d - 1, view, recv_z.at[n, d - 1], peer_z(d))

    def stage_d(n):
        loads[chunks + n][0].wait()

        def theirs(k, carry):
            inner = pl.ds(pl.multiple_of(k * tile, tile), tile)
            cols = pl.ds(pl.multiple_of(n * width + k * tile, tile), tile)
            send_d[n, :, inner] = down(at(1 - e, half), cols).astype(jnp.bfloat16)
            return carry

        lax.fori_loop(0, width // tile, theirs, 0)
        go(reduce_d(n))

        def ours(k, carry):
            cols = pl.ds(pl.multiple_of(n * width + k * tile, tile), tile)
            part[:, cols] = down(at(e, half), cols)
            return carry

        lax.fori_loop(0, width // tile, ours, 0)

    def stage_q(n):
        reduce_d(n).wait_recv()
        cols = pl.ds(n * width, width)
        away = at(1 - q, quarter)
        send_q[n] = (part[away, cols] + recv_d[n, away, :].astype(jnp.float32)).astype(jnp.bfloat16)
        go(reduce_q(n))
        stay = at(q, quarter)
        part[stay, cols] += recv_d[n, stay, :].astype(jnp.float32)

    def stage_p(n):
        reduce_q(n).wait_recv()
        cols = pl.ds(n * width, width)
        away = at(2 * q + 1 - p, eighth)
        send_p[n] = (part[away, cols] + recv_q[n, at(1 - p, eighth), :].astype(jnp.float32)).astype(
            jnp.bfloat16
        )
        go(reduce_p(n))
        stay = at(2 * q + p, eighth)
        part[stay, cols] += recv_q[n, at(p, eighth), :].astype(jnp.float32)

    def stage_z(n):
        reduce_p(n).wait_recv()
        cols = pl.ds(n * width, width)
        stay = at(2 * q + p, eighth)
        summed = part[stay, cols] + recv_p[n].astype(jnp.float32)
        send_z[n] = summed.astype(jnp.bfloat16)
        for d in range(1, depth):
            go(reduce_z(n, d))
        part[stay, cols] = summed

    def stage_out(n):
        cols = pl.ds(n * width, width)
        mixture = part[at((2 * q + p) * depth + z, own), cols]
        for d in range(1, depth):
            reduce_z(n, d).wait_recv()
            mixture += recv_z[n, d - 1].astype(jnp.float32)
        out_ref[:, cols] = (hidden_ref[:, cols].astype(jnp.float32) + mixture).astype(jnp.bfloat16)

    stages = (stage_d, stage_q, stage_p, stage_z, stage_out)
    for t in range(chunks + len(stages) - 1):
        for lag, stage in enumerate(stages):
            if 0 <= t - lag < chunks:
                stage(t - lag)
    for copy in started:
        copy.wait_send()


def body(depth, chunks, hidden_in, routes, norm_gain, router, w_gate, w_up, w_down):
    own, features = hidden_in.shape
    local, _, units = w_gate.shape
    width = features // chunks
    total = own * depth * 8
    half, quarter, eighth = total // 2, total // 4, total // 8
    slots = 2 * chunks * (depth - 1 + 3)
    bf16, f32 = jnp.bfloat16, jnp.float32
    vmem = pl.BlockSpec(memory_space=pltpu.VMEM)
    hbm = pl.BlockSpec(memory_space=pl.ANY)
    return pl.pallas_call(
        functools.partial(kernel, (depth, chunks, width, own)),
        out_shape=jax.ShapeDtypeStruct((own, features), bf16),
        in_specs=[vmem] * 4 + [hbm] * 3,
        out_specs=vmem,
        scratch_shapes=[
            pltpu.VMEM((2, local, features, units), bf16),
            pltpu.VMEM((local, units, features), bf16),
            pltpu.VMEM((total, features + LANES), bf16),
            pltpu.VMEM((2 * local, total, units), f32),
            pltpu.VMEM((local, total, units), bf16),
            pltpu.VMEM((half, features), f32),
            pltpu.VMEM((chunks, half, width), bf16),
            pltpu.VMEM((chunks, half, width), bf16),
            pltpu.VMEM((chunks, quarter, width), bf16),
            pltpu.VMEM((chunks, quarter, width), bf16),
            pltpu.VMEM((chunks, eighth, width), bf16),
            pltpu.VMEM((chunks, eighth, width), bf16),
            pltpu.VMEM((chunks, eighth, width), bf16),
            pltpu.VMEM((chunks, depth - 1, own, width), bf16),
            pltpu.SemaphoreType.DMA((slots,)),
            pltpu.SemaphoreType.DMA((slots,)),
            pltpu.SemaphoreType.DMA((3 * chunks,)),
        ],
        compiler_params=pltpu.CompilerParams(
            collective_id=0, has_side_effects=True, vmem_limit_bytes=66_000_000
        ),
    )(hidden_in, routes, norm_gain.reshape(1, -1), router.T, w_gate, w_up, w_down)


def solution(mesh):
    depth = mesh.shape["stream"] // 4
    assert mesh.shape["stream"] == 4 * depth and mesh.shape["expert"] == 2
    return jax.shard_map(
        functools.partial(body, depth, 4),
        mesh=mesh,
        in_specs=(
            P(("group", "stream", "expert"), None),
            P(("group", "stream", "expert"), None),
            P(),
            P(),
            P("expert", None, "stream"),
            P("expert", None, "stream"),
            P("expert", "stream", None),
        ),
        out_specs=P(("group", "stream", "expert"), None),
        check_vma=False,
    )
```
